32 devices in a mesh: xz: 16 (over z, y, x), gy: 2 (over core).
Axes of the slice: x: 2, y: 2, z: 4, core: 2. Of those that a mesh axis runs over, the one named last changes fastest.
Arguments:
- initial_state: float32 [3, 2, 16, 512, 512], P(None, None, 'gy', 'xz'), may hold values from -6 to 6
- drag_rate: float32 [16, 512, 1024], P('gy', 'xz'), may hold values from 0.02 to 0.6
- wall_control: float32 [512, 1024], P('xz'), may hold values from -6 to 6
- lift_profile: float32 [16], replicated, may hold values from 0.05 to 0.3
- schur_inverse: float32 [16, 8, 512, 512], P('gy', None, 'xz'), may hold values from -1 to 3, as said below
Outputs:
- final_state: float32 [3, 2, 16, 512, 512], P(None, None, 'gy', 'xz')
- control_gradient: float32 [512, 1024], P('xz', 'gy')
The draws below stay inside these ranges and needn't reach their ends.
Inputs may be any that keep to these rules, and one draw needn't show every extreme that they name: `schur_inverse`: each 8 x 8 block of one wavenumber holds the precomputed inverse of a Schur complement; dimension 1 indexes the block's columns.
All inputs are finite; a program needn't handle non-finite values.
Results may differ from the reference program's by a relative error of at most 0.00014.
Values sent between devices are 32-bit elements; how exact they have to be, the bound alone decides.
No kernel may reach another device: no remote copies, remote signals or barrier semaphores. Data moves between devices by JAX's collectives and lax.ppermute only.
A program may use at most 128 MiB of HBM per device.

```python
import math
import jax
import jax.numpy as jnp
from jax import lax

NX = 1024
NZ = 512
KX = 512
CY = 8
NY = 16
STEPS = 2
N_GY = 2


def draw_schur_inverse(key, part):
    subkeys = jax.random.split(key, 4)
    blocks = NY // CY
    full_shape = (blocks, CY, CY, NX // 2, NZ)
    diag_low = 0.4
    rank_weight = 0.6
    spread = 0.5
    diagonal = jax.random.uniform(subkeys[0], (blocks, CY, 1, NX // 2, NZ), jnp.float32, diag_low, 1.0)
    identity = (jnp.arange(CY)[:, None] == jnp.arange(CY)[None, :]).astype(jnp.float32)[None, :, :, None, None]
    jitter = jax.random.uniform(subkeys[1], full_shape, jnp.float32, -1.0, 1.0) * (spread / math.sqrt(CY))
    left_side = jax.random.uniform(subkeys[2], (blocks, CY, 1, NX // 2, NZ), jnp.float32, 0.5, 1.0)
    right_side = jax.random.uniform(subkeys[3], (blocks, 1, CY, NX // 2, NZ), jnp.float32, 0.5, 1.0)
    blocked = identity * diagonal + jitter + rank_weight * left_side * right_side
    stream_wave = 2.0 * math.pi / NX * jnp.arange(NX // 2).astype(jnp.float32)
    span_ids = jnp.arange(NZ)
    signed = jnp.where(span_ids < NZ // 2, span_ids, span_ids - NZ)
    span_wave = jnp.where(span_ids == NZ // 2, 0.0, 2.0 * math.pi / NZ * signed.astype(jnp.float32))
    damping = 1.0 + stream_wave[:, None] ** 2 + span_wave[None, :] ** 2
    return (blocked / damping).reshape(NY, CY, NX // 2, NZ)


def level_of(own_key, extent, cuts, least, top_value):
    gain = 1.0
    for axis_at, blocks in cuts:
        steps = jax.random.uniform(jax.random.fold_in(jax.random.fold_in(own_key, 6), axis_at), (blocks,), jnp.float32, least / len(cuts), top_value / len(cuts))
        gain = gain * jnp.repeat(jnp.exp(steps), extent[axis_at] // blocks).reshape((-1,) + (1,) * (len(extent) - 1 - axis_at))
    return gain


def gaussian(rng, shape, width, reach, cuts=(), dtype=jnp.bfloat16):
    level = level_of(rng, shape, cuts, -0.22, 0.18) if cuts else 1.0
    entries = jax.random.normal(rng, shape, jnp.float32) * width * level
    return jnp.minimum(jnp.maximum(entries, -reach), reach).astype(dtype)


def setup_inputs(seed: int = 0) -> dict:
    seeds = jax.random.split(jax.random.key(seed), 6)
    return {
        "initial_state": gaussian(seeds[0], (3, 2, NY, KX, NZ), 1.0, 6.0, ((2, 2), (3, 16)), jnp.float32),
        "drag_rate": jnp.clip(jnp.exp(math.log(0.6) - 3.4011974 * jax.random.uniform(seeds[1], (NY, NZ, NX), jnp.float32) ** level_of(seeds[1], (NY, NZ, NX), ((0, 2), (1, 16)), -0.2, 0.2)), 0.02, 0.6),
        "wall_control": gaussian(seeds[2], (NZ, NX), 1.0, 6.0, ((0, 16),), jnp.float32),
        "lift_profile": jnp.clip(jnp.exp(jax.random.uniform(seeds[3], (NY,), jnp.float32, math.log(0.05), math.log(0.3))), 0.05, 0.3),
        "schur_inverse": draw_schur_inverse(jax.random.fold_in(seeds[5], 71), 0),
    }


DIFFUSION = 0.04

def pair_rotate(spectrum, factor):
    return jnp.stack([-factor * spectrum[1], factor * spectrum[0]])

def reference(initial_state, drag_rate, wall_control, lift_profile, schur_inverse):
    mode_ids = jnp.arange(KX)
    stream_factor = (2.0 * math.pi / NX * mode_ids.astype(jnp.float32))[:, None]
    span_ids = jnp.arange(NZ)
    signed = jnp.where(span_ids < NZ // 2, span_ids, span_ids - NZ)
    span_wave = jnp.where(span_ids == NZ // 2, 0.0, 2.0 * math.pi / NZ * signed.astype(jnp.float32))
    wave_square = stream_factor ** 2 + span_wave[None, :] ** 2

    def to_physical(spectral):
        values = lax.complex(spectral[0], spectral[1])
        values = jnp.fft.ifft(values, axis=2, norm='ortho')
        values = jnp.swapaxes(values, 1, 2)
        values = jnp.pad(values, ((0, 0), (0, 0), (0, 1)))
        return jnp.fft.irfft(values, n=NX, axis=2, norm='ortho')

    def to_spectral(physical):
        values = jnp.fft.rfft(physical, axis=2, norm='ortho')[:, :, :KX]
        values = jnp.swapaxes(values, 1, 2)
        values = jnp.fft.fft(values, axis=2, norm='ortho')
        return jnp.stack([jnp.real(values), jnp.imag(values)])

    def curvature(spectrum):
        padded = jnp.pad(spectrum, ((0, 0), (1, 1), (0, 0), (0, 0)))
        return padded[:, 2:] - 2.0 * spectrum + padded[:, :-2]

    def centred(spectrum):
        padded = jnp.pad(spectrum, ((0, 0), (1, 1), (0, 0), (0, 0)))
        return (padded[:, 2:] - padded[:, :-2]) / 2.0

    def solve(source):
        running = jnp.zeros((2, KX, NZ), jnp.float32)
        partials = []
        for block_index in range(N_GY):
            matrix = schur_inverse[block_index * CY:(block_index + 1) * CY]
            values = source[:, block_index * CY:(block_index + 1) * CY]
            summed = jnp.einsum('ijkq,cjkq->cikq', matrix, values, precision=lax.Precision.HIGHEST)
            partial_value = summed + matrix[:, 0][None] * running[:, None]
            running = partial_value[:, CY - 1]
            partials.append(partial_value)
        running = jnp.zeros((2, KX, NZ), jnp.float32)
        solved = [None] * N_GY
        for block_index in reversed(range(N_GY)):
            matrix = schur_inverse[block_index * CY:(block_index + 1) * CY]
            complete = partials[block_index] + matrix[:, CY - 1][None] * running[:, None]
            running = complete[:, 0]
            solved[block_index] = complete
        return jnp.concatenate(solved, axis=1)

    def evolve(control_plane):
        control_hat = to_spectral(control_plane[None])[:, 0]
        fields = initial_state
        for section_index in range(STEPS):
            stream_part = fields[0]
            normal_part = fields[1]
            span_part = fields[2]
            drag_term = to_spectral(drag_rate * to_physical(stream_part))
            stream_star = stream_part + DIFFUSION * (curvature(stream_part) - wave_square * stream_part) - drag_term
            normal_star = normal_part + DIFFUSION * (curvature(normal_part) - wave_square * normal_part) + lift_profile[:, None, None] * control_hat[:, None]
            span_star = span_part + DIFFUSION * (curvature(span_part) - wave_square * span_part)
            divergence = pair_rotate(stream_star, stream_factor) + centred(normal_star) + pair_rotate(span_star, span_wave)
            pressure = solve(divergence)
            fields = jnp.stack([stream_star - pair_rotate(pressure, stream_factor), normal_star - centred(pressure), span_star - pair_rotate(pressure, span_wave)])
        return fields
    final_state, pullback = jax.vjp(evolve, wall_control)
    control_gradient = pullback(final_state)[0]
    return (final_state, control_gradient)
```

```python
import math

import jax
import jax.numpy as jnp
import ml_dtypes
import numpy as np
from jax import lax
from jax.experimental import pallas as pl
from jax.experimental.pallas import tpu as pltpu
from jax.sharding import PartitionSpec as P

STEPS = 2
DIFFUSION = 0.04
LANES = 128


def split_constant(table):
    high = table.astype(ml_dtypes.bfloat16)
    low = (table - high.astype(np.float64)).astype(ml_dtypes.bfloat16)
    return high, low


def span_tables(span_count):
    ids = np.arange(span_count)
    angle = 2.0 * np.pi / span_count * (np.outer(ids, ids) % span_count)
    scale = 1.0 / np.sqrt(span_count)
    return split_constant(np.cos(angle) * scale) + split_constant(np.sin(angle) * scale)


def stream_tables(stream_len, member_count, mode_count):
    modes = np.arange(member_count * mode_count)
    angle = 2.0 * np.pi / stream_len * (np.outer(np.arange(stream_len), modes) % stream_len)
    pair = np.stack([np.cos(angle), -np.sin(angle)], axis=1) / np.sqrt(stream_len)
    pair = pair.reshape(stream_len, 2, member_count, mode_count).transpose(0, 2, 1, 3)
    pair = pair.reshape(stream_len, -1)
    return split_constant(pair) + split_constant(np.ascontiguousarray(pair.T))


def halves(x):
    high = x.astype(jnp.bfloat16)
    low = (x - high.astype(jnp.float32)).astype(jnp.bfloat16)
    return high, low


def dot(a, b):
    return jnp.dot(a, b, preferred_element_type=jnp.float32)


def dot3(a, b):
    return dot(a[0], b[0]) + (dot(a[0], b[1]) + dot(a[1], b[0]))


def outside_halves(x):
    high = lax.reduce_precision(x, 8, 7)
    return high.astype(jnp.bfloat16), (x - high).astype(jnp.bfloat16)


def slot_ids(rows, width):
    return lax.broadcasted_iota(jnp.int32, (rows, LANES), 1) // width


def pick(slots, tiles, offset):
    count = len(tiles)
    chosen = tiles[0]
    for index in range(1, count):
        chosen = jnp.where(slots == (index + offset) % count, tiles[index], chosen)
    return chosen


def turn(tile, amount):
    amount = amount % LANES
    return pltpu.roll(tile, amount, 1) if amount else tile


def pack_kernel(rows, modes, spans, width, s_ref, weight_ref, ch, cl, sh, sl, out_ref):
    group = LANES // width
    weight = weight_ref[...]
    slots = slot_ids(modes, width)
    cos = (ch[...], cl[...])
    sin = (sh[...], sl[...])
    for high_row in range(rows // group):
        near = slice(high_row * group, (high_row + 1) * group)
        real = halves(s_ref[0, near].reshape(group * modes, spans))
        imag = halves(s_ref[1, near].reshape(group * modes, spans))
        parts = (dot3(real, cos) - dot3(imag, sin), dot3(real, sin) + dot3(imag, cos))
        for part in range(2):
            for tile in range(spans // LANES):
                rolled = [
                    turn(
                        parts[part][j * modes : (j + 1) * modes, tile * LANES : (tile + 1) * LANES] * weight,
                        width * j,
                    )
                    for j in range(group)
                ]
                for e in range(group):
                    out_ref[
                        tile * group + e,
                        part * modes : (part + 1) * modes,
                        high_row * LANES : (high_row + 1) * LANES,
                    ] = turn(pick(slots, rolled, e), -width * e)


def unpack_kernel(rows, modes, spans, width, r_ref, weight_ref, ch, cl, sh, sl, out_ref, x_ref):
    group = LANES // width
    weight = weight_ref[...]
    slots = slot_ids(modes, width)
    cos = (ch[...], cl[...])
    sin = (sh[...], sl[...])
    for high_row in range(rows // group):
        for part in range(2):
            for tile in range(spans // LANES):
                rolled = [
                    turn(
                        r_ref[
                            tile * group + e,
                            part * modes : (part + 1) * modes,
                            high_row * LANES : (high_row + 1) * LANES,
                        ]
                        * weight,
                        width * e,
                    )
                    for e in range(group)
                ]
                for j in range(group):
                    x_ref[
                        part, j * modes : (j + 1) * modes, tile * LANES : (tile + 1) * LANES
                    ] = turn(pick(slots, rolled, j), -width * j)
        real = halves(x_ref[0])
        imag = halves(x_ref[1])
        near = slice(high_row * group, (high_row + 1) * group)
        shape = (group, modes, spans)
        out_ref[0, near] = (dot3(real, cos) + dot3(imag, sin)).reshape(shape)
        out_ref[1, near] = (dot3(imag, cos) - dot3(real, sin)).reshape(shape)


def stream_kernel(r_ref, drag_ref, ih, il, fh, fl, out_ref, high_ref, low_ref):
    @pl.when(pl.program_id(0) == 0)
    def _():
        high, low = halves(r_ref[...])
        high_ref[...] = high
        low_ref[...] = low
        out_ref[...] = jnp.zeros_like(out_ref)

    physical = dot3((ih[...], il[...]), (high_ref[...], low_ref[...]))
    out_ref[...] += dot3((fh[...], fl[...]), halves(drag_ref[...] * physical))


def per_device(initial_state, drag_rate, wall_control, lift_profile, schur_inverse):
    row_count = initial_state.shape[2]
    mode_count = initial_state.shape[3]
    span_count = initial_state.shape[4]
    stream_len = drag_rate.shape[2]
    width = drag_rate.shape[1]
    member_count = lax.axis_size("xz")
    slab_count = lax.axis_size("gy")
    slab_index = lax.axis_index("gy")
    pencil_index = lax.axis_index("xz")
    lane_count = row_count * width
    pair_count = 2 * mode_count
    last_row = row_count - 1
    z_tables = tuple(jnp.asarray(t) for t in span_tables(span_count))
    inv_high, inv_low, fwd_high, fwd_low = (
        jnp.asarray(t) for t in stream_tables(stream_len, member_count, mode_count)
    )
    cos_z, sin_z = z_tables[:2], z_tables[2:]
    mode_ids = pencil_index * mode_count + jnp.arange(mode_count)
    stream_factor = (2.0 * math.pi / stream_len * mode_ids.astype(jnp.float32))[:, None]
    mode_weight = jnp.where(mode_ids == 0, 1.0, 2.0).astype(jnp.float32)[:, None]
    no_weight = jnp.ones_like(mode_weight)
    span_ids = jnp.arange(span_count)
    signed = jnp.where(span_ids < span_count // 2, span_ids, span_ids - span_count)
    span_wave = jnp.where(
        span_ids == span_count // 2, 0.0, 2.0 * math.pi / span_count * signed.astype(jnp.float32)
    )
    wave_square = stream_factor**2 + span_wave[None, :] ** 2
    has_prev = slab_index > 0
    has_next = slab_index < slab_count - 1

    def exchange(block):
        return lax.all_to_all(block, "xz", split_axis=0, concat_axis=0, tiled=True)

    def plain_pack(s, weight):
        rows = s.shape[1]
        real = outside_halves(s[0].reshape(-1, span_count))
        imag = outside_halves(s[1].reshape(-1, span_count))
        parts = jnp.stack(
            [dot3(real, cos_z) - dot3(imag, sin_z), dot3(real, sin_z) + dot3(imag, cos_z)]
        ).reshape(2, rows, mode_count, member_count, width)
        parts = parts * weight[None, None, :, None]
        return parts.transpose(3, 0, 2, 1, 4).reshape(member_count, pair_count, rows * width)

    def plain_unpack(block, weight):
        rows = block.shape[2] // width
        block = block.reshape(member_count, 2, mode_count, rows, width).transpose(1, 3, 2, 0, 4)
        block = block * weight[None, None, :, None]
        real = outside_halves(block[0].reshape(-1, span_count))
        imag = outside_halves(block[1].reshape(-1, span_count))
        parts = [dot3(real, cos_z) + dot3(imag, sin_z), dot3(imag, cos_z) - dot3(real, sin_z)]
        return jnp.stack(parts).reshape(2, rows, mode_count, span_count)

    group = LANES // width if LANES % width == 0 else 0
    tiled = (
        group > 0
        and row_count % group == 0
        and mode_count % 8 == 0
        and span_count % LANES == 0
    )
    sizes = (row_count, mode_count, span_count, width)

    def pack(s, weight):
        if not tiled:
            return plain_pack(s, weight)
        return pl.pallas_call(
            lambda *refs: pack_kernel(*sizes, *refs),
            out_shape=jax.ShapeDtypeStruct((member_count, pair_count, lane_count), jnp.float32),
            name="pack",
        )(s, weight, *z_tables)

    def unpack(block, weight):
        if not tiled:
            return plain_unpack(block, weight)
        return pl.pallas_call(
            lambda *refs: unpack_kernel(*sizes, *refs),
            out_shape=jax.ShapeDtypeStruct((2, row_count, mode_count, span_count), jnp.float32),
            scratch_shapes=[pltpu.VMEM((2, group * mode_count, span_count), jnp.float32)],
            name="unpack",
        )(block, weight, *z_tables)

    all_pairs = member_count * pair_count
    drag_turned = drag_rate.reshape(lane_count, stream_len).T
    step = min(256, stream_len)

    def stream(block):
        return pl.pallas_call(
            stream_kernel,
            grid=(stream_len // step,),
            in_specs=[
                pl.BlockSpec((all_pairs, lane_count), lambda i: (0, 0)),
                pl.BlockSpec((step, lane_count), lambda i: (i, 0)),
                pl.BlockSpec((step, all_pairs), lambda i: (i, 0)),
                pl.BlockSpec((step, all_pairs), lambda i: (i, 0)),
                pl.BlockSpec((all_pairs, step), lambda i: (0, i)),
                pl.BlockSpec((all_pairs, step), lambda i: (0, i)),
            ],
            out_specs=pl.BlockSpec((all_pairs, lane_count), lambda i: (0, 0)),
            out_shape=jax.ShapeDtypeStruct((all_pairs, lane_count), jnp.float32),
            scratch_shapes=[pltpu.VMEM((all_pairs, lane_count), jnp.bfloat16)] * 2,
            name="stream",
        )(block, drag_turned, inv_high, inv_low, fwd_high, fwd_low)

    def drag(s, before, after):
        block = exchange(pack(s, before)).reshape(all_pairs, lane_count)
        block = stream(block).reshape(member_count, pair_count, lane_count)
        return unpack(exchange(block), after)

    def rotate(spectrum, factor):
        return jnp.stack([-factor * spectrum[1], factor * spectrum[0]])

    padded_lift = jnp.pad(lift_profile, 1)
    lift_near = lax.dynamic_slice_in_dim(padded_lift, slab_index * row_count, row_count + 2)
    lift_own = lift_near[1 : row_count + 1]

    up = [(i, i + 1) for i in range(slab_count - 1)]
    down = [(i + 1, i) for i in range(slab_count - 1)]

    def neighbours(fields):
        tail = jnp.stack(
            [fields[0][:, last_row], fields[2][:, last_row], fields[1][:, last_row - 1], fields[1][:, last_row]]
        )
        head = jnp.stack([fields[0][:, 0], fields[2][:, 0], fields[1][:, 0], fields[1][:, 1]])
        return lax.ppermute(tail, "gy", up), lax.ppermute(head, "gy", down)

    def laplace(wide):
        mid = wide[:, 1:-1]
        return mid + DIFFUSION * (wide[:, 2:] - 2.0 * mid + wide[:, :-2] - wave_square * mid)

    def advance(fields, rims, drag_term, control_hat):
        before, behind = rims
        u_wide = jnp.concatenate([before[0][:, None], fields[0], behind[0][:, None]], axis=1)
        w_wide = jnp.concatenate([before[1][:, None], fields[2], behind[1][:, None]], axis=1)
        v_wide = jnp.concatenate(
            [before[2][:, None], before[3][:, None], fields[1], behind[2][:, None], behind[3][:, None]],
            axis=1,
        )
        v_star = laplace(v_wide)
        if control_hat is not None:
            v_star = v_star + lift_near[:, None, None] * control_hat[:, None]
        first = jnp.where(has_prev, v_star[:, 0], 0.0)
        final = jnp.where(has_next, v_star[:, -1], 0.0)
        rim = jnp.concatenate([first[:, None], v_star[:, 1:-1], final[:, None]], axis=1)
        slope = 0.5 * (rim[:, 2:] - rim[:, :-2])
        return (laplace(u_wide) - drag_term, v_star[:, 1:-1], laplace(w_wide)), slope

    corner_own = jnp.stack(
        [
            schur_inverse[last_row, 0],
            schur_inverse[0, 0],
            schur_inverse[0, last_row],
            schur_inverse[last_row, last_row],
        ]
    )
    corners = lax.all_gather(corner_own[None], "gy", axis=0, tiled=True)

    def solve(source, transposed):
        direct = jnp.zeros_like(source)
        for column in range(row_count):
            factor = schur_inverse[column] if transposed else schur_inverse[:, column]
            direct = direct + factor[None] * source[:, column : column + 1]
        if transposed:
            first_column = schur_inverse[0]
            last_column = schur_inverse[last_row]
        else:
            first_column = schur_inverse[:, 0]
            last_column = schur_inverse[:, last_row]
        ratio_at, turn_at = (2, 0) if transposed else (0, 2)
        ends = jnp.stack([direct[:, last_row], direct[:, 0]])
        ends = lax.all_gather(ends[None], "gy", axis=0, tiled=True)
        nothing = jnp.zeros_like(direct[:, 0])
        running = nothing
        before = []
        for member in range(slab_count):
            before.append(running)
            running = ends[member, 0] + corners[member, ratio_at][None] * running
        running = nothing
        behind = [nothing] * slab_count
        for member in reversed(range(slab_count)):
            behind[member] = running
            top = ends[member, 1] + corners[member, 1][None] * before[member]
            running = top + corners[member, turn_at][None] * running
        entering, leaving = before[0], behind[0]
        corner = jnp.zeros_like(corners[0, 3])
        for member in range(1, slab_count):
            here = slab_index == member
            entering = jnp.where(here, before[member], entering)
            leaving = jnp.where(here, behind[member], leaving)
            corner = jnp.where(here, corners[member - 1, 3], corner)
        pressure = direct + first_column[None] * entering[:, None] + last_column[None] * leaving[:, None]
        above = jnp.where(has_prev, entering + corner[None] * pressure[:, 0], 0.0)
        wide = jnp.concatenate([above[:, None], pressure, leaving[:, None]], axis=1)
        return pressure, 0.5 * (wide[:, 2:] - wide[:, :-2])

    def project(fields, normal_slope, transposed):
        divergence = rotate(fields[0], stream_factor) + normal_slope + rotate(fields[2], span_wave)
        pressure, pressure_slope = solve(divergence, transposed)
        return (
            fields[0] - rotate(pressure, stream_factor),
            fields[1] - pressure_slope,
            fields[2] - rotate(pressure, span_wave),
        )

    control = outside_halves(wall_control.T)
    control_half = dot3((fwd_high, fwd_low), control).reshape(member_count, pair_count, width)
    control_hat = plain_unpack(exchange(control_half), no_weight)[:, 0]

    fields = (initial_state[0], initial_state[1], initial_state[2])
    for _ in range(STEPS):
        rims = neighbours(fields)
        drag_term = drag(fields[0], mode_weight, no_weight)
        provisional, slope = advance(fields, rims, drag_term, control_hat)
        fields = project(provisional, slope, False)
    final_state = jnp.stack(fields)
    before = lax.ppermute(fields[1][:, last_row:], "gy", up)
    behind = lax.ppermute(fields[1][:, :1], "gy", down)
    seed = jnp.concatenate([before, fields[1], behind], axis=1)
    slope = 0.5 * (seed[:, 2:] - seed[:, :-2])
    costate = fields
    wall_sum = jnp.zeros_like(control_hat)
    for section in range(STEPS):
        projected = project(costate, slope, True)
        wall_sum = wall_sum + jnp.sum(lift_own[:, None, None] * projected[1], axis=1)
        if section + 1 < STEPS:
            rims = neighbours(projected)
            drag_term = drag(projected[0], no_weight, mode_weight)
            costate, slope = advance(projected, rims, drag_term, None)
    block = exchange(plain_pack(wall_sum[:, None], no_weight)).reshape(all_pairs, width)
    block = outside_halves(block.T)
    wall_plane = dot3(block, (fwd_high, fwd_low))
    control_gradient = lax.psum_scatter(wall_plane, "gy", scatter_dimension=1, tiled=True)
    return (final_state, control_gradient)


def solution(mesh):
    return jax.shard_map(
        per_device,
        mesh=mesh,
        in_specs=(
            P(None, None, "gy", "xz", None),
            P("gy", "xz", None),
            P("xz", None),
            P(),
            P("gy", None, "xz", None),
        ),
        out_specs=(P(None, None, "gy", "xz", None), P("xz", "gy")),
        check_vma=False,
    )
```
